32 devices in a mesh: zero: 8 (over y, x, core), tp: 4 (over z).
Axes of the slice: x: 2, y: 2, z: 4, core: 2. Of those that a mesh axis runs over, the one named last changes fastest.
Arguments:
- weight_gate: bfloat16 [2560, 9728], P('zero', 'tp'), may hold values from -0.125 to 0.125
- low_gate: bfloat16 [2560, 16], P('zero'), may hold values from -0.125 to 0.125
- high_gate: bfloat16 [16, 9728], P(None, 'tp'), may hold values from -1.5 to 1.5
- weight_up: bfloat16 [2560, 9728], P('zero', 'tp'), may hold values from -0.125 to 0.125
- low_up: bfloat16 [2560, 16], P('zero'), may hold values from -0.125 to 0.125
- high_up: bfloat16 [16, 9728], P(None, 'tp'), may hold values from -1.5 to 1.5
- weight_down: bfloat16 [9728, 2560], P('tp', 'zero'), may hold values from -0.0625 to 0.0625
- low_down: bfloat16 [9728, 16], P('tp'), may hold values from -0.0625 to 0.0625
- high_down: bfloat16 [16, 2560], P(None, 'zero'), may hold values from -1.5 to 1.5
- norm_train: float32 [2560], P(('zero', 'tp')), may hold values from 0.25 to 1.75
- norm_step: float32 [2560], P(('zero', 'tp')), may hold values from -0.3 to 0.3
Outputs:
- ready_gate: bfloat16 [2560, 9728], P(None, 'tp')
- ready_up: bfloat16 [2560, 9728], P(None, 'tp')
- ready_down: bfloat16 [9728, 2560], P('tp')
- serve_norm: bfloat16 [2560], replicated
The draws below stay inside these ranges and needn't reach their ends.
All inputs are finite; a program needn't handle non-finite values.
Results may differ from the reference program's by a relative error of at most 0.001.
Values may be sent and summed in bfloat16 or wider, within the bound.
A program may use at most 128 MiB of HBM per device.

```python
import jax
import jax.numpy as jnp

D_MODEL = 2560
D_INNER = 9728
RANK = 16


def shard_levels(own_key, dims, shards, low, top_value):
    def one(dim, parts):
        steps = jax.random.uniform(jax.random.fold_in(jax.random.fold_in(own_key, 6), dim), (parts,), jnp.float32, low / len(shards), top_value / len(shards))
        return jnp.repeat(jnp.exp(steps), dims[dim] // parts).reshape((-1,) + (1,) * (len(dims) - dim - 1))

    loudness = one(*shards[0])
    for cut in shards[1:]:
        loudness = loudness * one(*cut)
    return loudness


def gaussian(stream_key, shape, spread, most, shards=(), kind=jnp.bfloat16):
    array = jax.random.normal(stream_key, shape, jnp.float32) * spread
    if len(shards) > 0:
        array = shard_levels(stream_key, shape, shards, -0.22, 0.18) * array
    return jnp.clip(array, min=-most, max=most).astype(kind)


def setup_inputs(seed: int = 0) -> dict:
    key_of = jax.random.split(jax.random.key(seed), 12)
    return {
        "weight_gate": gaussian(key_of[0], (D_MODEL, D_INNER), D_MODEL ** -0.5, 0.125, ((0, 8), (1, 4))),
        "low_gate": gaussian(key_of[1], (D_MODEL, RANK), D_MODEL ** -0.5, 0.125, ((0, 8),)),
        "high_gate": gaussian(key_of[2], (RANK, D_INNER), RANK ** -0.5, 1.5, ((1, 4),)),
        "weight_up": gaussian(key_of[3], (D_MODEL, D_INNER), D_MODEL ** -0.5, 0.125, ((0, 8), (1, 4))),
        "low_up": gaussian(key_of[4], (D_MODEL, RANK), D_MODEL ** -0.5, 0.125, ((0, 8),)),
        "high_up": gaussian(key_of[5], (RANK, D_INNER), RANK ** -0.5, 1.5, ((1, 4),)),
        "weight_down": gaussian(key_of[6], (D_INNER, D_MODEL), D_INNER ** -0.5, 0.0625, ((0, 4), (1, 8))),
        "low_down": gaussian(key_of[7], (D_INNER, RANK), D_INNER ** -0.5, 0.0625, ((0, 4),)),
        "high_down": gaussian(key_of[8], (RANK, D_MODEL), RANK ** -0.5, 1.5, ((1, 8),)),
        "norm_train": jnp.clip(1.0 + 0.15 * jax.random.normal(key_of[9], (D_MODEL,), jnp.float32), 0.25, 1.75),
        "norm_step": jnp.clip(jax.random.uniform(key_of[10], (D_MODEL,), jnp.float32, -0.3, 0.3) * shard_levels(key_of[10], (D_MODEL,), ((0, 32),), -0.4, 0.0), -0.3, 0.3),
    }


mix_rate = 0.5


def reference(weight_gate, low_gate, high_gate, weight_up, low_up, high_up, weight_down, low_down, high_down, norm_train, norm_step):
    latest_gate = weight_gate.astype(jnp.float32) + mix_rate * jnp.dot(low_gate, high_gate, preferred_element_type=jnp.float32)
    latest_up = weight_up.astype(jnp.float32) + mix_rate * jnp.dot(low_up, high_up, preferred_element_type=jnp.float32)
    latest_down = weight_down.astype(jnp.float32) + mix_rate * jnp.dot(low_down, high_down, preferred_element_type=jnp.float32)
    ready_gate = latest_gate.astype(jnp.bfloat16)
    ready_up = latest_up.astype(jnp.bfloat16)
    ready_down = latest_down.astype(jnp.bfloat16)
    serve_norm = (norm_train + norm_step).astype(jnp.bfloat16)
    return ready_gate, ready_up, ready_down, serve_norm
```

```python
import functools

import jax
import jax.numpy as jnp
from jax import lax
from jax.experimental import pallas as pl
from jax.experimental.pallas import tpu as pltpu
from jax.sharding import PartitionSpec as P

mix_rate = 0.5
MESH = pl.DeviceIdType.MESH
LANES = 128
CHUNKS = 4
GROUP = 8


def merge_rows(weight, factor, other):
    product = lax.dot_general(
        factor, other, (((0,), (0,)), ((), ())), preferred_element_type=jnp.float32
    )
    return (weight.astype(jnp.float32) + mix_rate * product).astype(jnp.bfloat16)


def gather_kernel(
    weight_down, factor_down, other_down,
    weight_gate, factor_gate, other_gate,
    weight_up, factor_up, other_up,
    gate, up, down, held,
    x_send, x_recv, y_send, y_recv, fx_send, fx_recv, fy_send, fy_recv, p_send, p_recv,
):
    rows, columns = weight_gate.shape
    step = rows // CHUNKS
    half = CHUNKS // 2
    me = lax.axis_index("zero")
    core = lax.rem(me, 2)
    x = lax.rem(lax.div(me, 2), 2)
    y = lax.div(me, 4)

    def at(yy, xx, cc):
        return (yy * 2 + xx) * 2 + cc

    partner = at(y, x, 1 - core)
    across_x = at(y, 1 - x, core)
    across_y = at(1 - y, x, core)
    across = at(1 - y, 1 - x, core)

    barrier = pltpu.get_barrier_semaphore()
    for peer in (partner, across_x, across_y):
        pl.semaphore_signal(barrier, inc=1, device_id={"zero": peer}, device_id_type=MESH)
    pl.semaphore_wait(barrier, 3)

    stacks = (held, gate, up)
    sources = (
        (weight_down, factor_down, other_down),
        (weight_gate, factor_gate, other_gate),
        (weight_up, factor_up, other_up),
    )

    def part(i, owner, c, count=1):
        first = pl.multiple_of(owner * rows + c * step, 16)
        return stacks[i].at[pl.ds(first, step * count), :]

    def copy(i, owner, c, peer, send, recv, count=1):
        ref = part(i, owner, c, count)
        return pltpu.make_async_remote_copy(
            src_ref=ref, dst_ref=ref, send_sem=send, recv_sem=recv,
            device_id={"zero": peer}, device_id_type=MESH,
        )

    def on_x(i, owner, c):
        return copy(i, owner, c, across_x, x_send.at[i, c], x_recv.at[i, c])

    def on_y(i, owner, c):
        return copy(i, owner, c, across_y, y_send.at[i, c], y_recv.at[i, c])

    def forward_x(i, owner, c):
        return copy(i, owner, c, across_x, fx_send.at[i, c - half], fx_recv.at[i, c - half])

    def forward_y(i, owner, c):
        return copy(i, owner, c, across_y, fy_send.at[i, c], fy_recv.at[i, c])

    def share(i, slot, owner, c):
        return copy(i, owner, c, partner, p_send.at[slot, i, c], p_recv.at[slot, i, c])

    early, late = range(half), range(half, CHUNKS)
    sent = []

    def go(dma):
        dma.start()
        sent.append(dma)

    for i in range(3):
        weight, factor, other = sources[i]
        first = pl.multiple_of(me * rows, 16)

        @pl.loop(0, columns // LANES)
        def _(t):
            cols = pl.ds(pl.multiple_of(t * LANES, LANES), LANES)
            stacks[i][pl.ds(first, rows), cols] = merge_rows(
                weight[:, cols], factor[...], other[:, cols]
            )

        for cx, cy in zip((*early, *late), (*late, *early)):
            go(on_x(i, me, cx))
            go(on_y(i, me, cy))
        for c in range(CHUNKS):
            go(share(i, 0, me, c))

    def turn(owner):
        base = pl.multiple_of(lax.div(owner, 2) * (2 * rows), LANES)

        @pl.loop(0, columns // LANES)
        def _(t):
            cols = pl.ds(pl.multiple_of(t * LANES, LANES), LANES)
            down[cols, pl.ds(base, 2 * rows)] = held[pl.ds(base, 2 * rows), cols].T

    def shared(i, slot, owner):
        other_core = owner + partner - me
        for c in range(CHUNKS):
            share(i, slot, other_core, c).wait_recv()

    for i in range(3):
        for c, d in zip(early, late):
            on_x(i, across_x, c).wait_recv()
            go(forward_y(i, across_x, c))
            go(share(i, 1, across_x, c))
            on_y(i, across_y, d).wait_recv()
            go(forward_x(i, across_y, d))
            go(share(i, 2, across_y, d))
        for c, d in zip(early, late):
            on_x(i, across_x, d).wait_recv()
            go(share(i, 1, across_x, d))
            on_y(i, across_y, c).wait_recv()
            go(share(i, 2, across_y, c))
        for slot, owner in ((0, me), (1, across_x), (2, across_y)):
            shared(i, slot, owner)
            if i == 0:
                turn(owner)
    for i in range(3):
        for c, d in zip(early, late):
            forward_y(i, across, c).wait_recv()
            go(share(i, 3, across, c))
            forward_x(i, across, d).wait_recv()
            go(share(i, 3, across, d))
        if i == 0:
            shared(i, 3, across)
            turn(across)
    for i in (1, 2):
        shared(i, 3, across)
    for dma in sent:
        dma.wait_send()


def gather(sources, names):
    rows, columns = sources[0].shape
    stack = (rows * GROUP, columns)
    turned = (columns, rows * GROUP)
    dma = pltpu.SemaphoreType.DMA
    half = CHUNKS // 2
    return pl.pallas_call(
        gather_kernel,
        out_shape=(
            pltpu.VMEM(stack, jnp.bfloat16),
            pltpu.VMEM(stack, jnp.bfloat16),
            pltpu.VMEM(turned, jnp.bfloat16),
        ),
        in_specs=[pl.BlockSpec(memory_space=pltpu.VMEM)] * 9,
        out_specs=[pl.BlockSpec(memory_space=pltpu.VMEM)] * 3,
        scratch_shapes=[
            pltpu.VMEM(stack, jnp.bfloat16),
            dma((3, CHUNKS)), dma((3, CHUNKS)), dma((3, CHUNKS)), dma((3, CHUNKS)),
            dma((3, half)), dma((3, half)), dma((3, half)), dma((3, half)),
            dma((4, 3, CHUNKS)), dma((4, 3, CHUNKS)),
        ],
        compiler_params=pltpu.CompilerParams(
            collective_id=0, has_side_effects=True, vmem_limit_bytes=20 * 2**20
        ),
        name="gather_merged",
    )(*sources)


def store_kernel(gate, up, down, gate_out, up_out, down_out, sems):
    pieces = 4
    copies = []
    for i, (src, dst) in enumerate(((gate, gate_out), (up, up_out), (down, down_out))):
        size = src.shape[0] // pieces
        for k in range(pieces):
            at = pl.ds(k * size, size)
            copies.append(pltpu.make_async_copy(src.at[at, :], dst.at[at, :], sems.at[i, k]))
            copies[-1].start()
    for copy in copies:
        copy.wait()


def store(gate, up, down):
    return pl.pallas_call(
        store_kernel,
        out_shape=tuple(jax.ShapeDtypeStruct(a.shape, a.dtype) for a in (gate, up, down)),
        in_specs=[pl.BlockSpec(memory_space=pltpu.VMEM)] * 3,
        out_specs=[pl.BlockSpec(memory_space=pl.ANY)] * 3,
        scratch_shapes=[pltpu.SemaphoreType.DMA((3, 4))],
        compiler_params=pltpu.CompilerParams(vmem_limit_bytes=2**20),
        name="store_merged",
    )(gate, up, down)


def local(
    weight_gate, low_gate, high_gate,
    weight_up, low_up, high_up,
    weight_down, low_down, high_down,
    norm_train, norm_step,
    *, fast,
):
    serve_norm = lax.all_gather(
        (norm_train + norm_step).astype(jnp.bfloat16), ("zero", "tp"), axis=0, tiled=True
    )
    sources = (
        (weight_down.T, high_down, low_down.T),
        (weight_gate, low_gate.T, high_gate),
        (weight_up, low_up.T, high_up),
    )
    if fast:
        ready_gate, ready_up, ready_down = store(*gather(sum(sources, ()), None))
    else:
        down, gate, up = (merge_rows(*s) for s in sources)
        ready_gate, ready_up, ready_down = (
            lax.all_gather(a, "zero", axis=0, tiled=True) for a in (gate, up, down)
        )
        ready_down = ready_down.T
    return (ready_gate, ready_up, ready_down, serve_norm)


def solution(mesh):
    def step(*args):
        zero, tp = mesh.shape["zero"], mesh.shape["tp"]
        rows, columns = args[0].shape[0] // zero, args[0].shape[1] // tp
        fast = (
            zero == GROUP
            and rows % (16 * CHUNKS) == 0
            and columns % LANES == 0
            and args[6].shape == args[0].shape[::-1]
        )
        return jax.shard_map(
            functools.partial(local, fast=fast),
            mesh=mesh,
            in_specs=(
                P("zero", "tp"), P("zero", None), P(None, "tp"),
                P("zero", "tp"), P("zero", None), P(None, "tp"),
                P("tp", "zero"), P("tp", None), P(None, "zero"),
                P(("zero", "tp")), P(("zero", "tp")),
            ),
            out_specs=(P(None, "tp"), P(None, "tp"), P("tp", None), P()),
            check_vma=False,
        )(*args)

    return step
```

```python
import functools

import jax
import jax.numpy as jnp
from jax import lax
from jax.experimental import pallas as pl
from jax.experimental.pallas import tpu as pltpu
from jax.sharding import PartitionSpec as P

mix_rate = 0.5
MESH = pl.DeviceIdType.MESH
LANES = 128
CHUNKS = 4
GROUP = 8


def merge_rows(weight, factor, other):
    product = lax.dot_general(
        factor, other, (((0,), (0,)), ((), ())), preferred_element_type=jnp.float32
    )
    return (weight.astype(jnp.float32) + mix_rate * product).astype(jnp.bfloat16)


def gather_kernel(
    tp,
    weight_down, factor_down, other_down,
    weight_gate, factor_gate, other_gate,
    weight_up, factor_up, other_up,
    norm_train, norm_step,
    gate, up, down, gains, stack, turned, out_sems,
    n_send, n_recv,
    x_send, x_recv, y_send, y_recv, fx_send, fx_recv, fy_send, fy_recv, p_send, p_recv,
):
    rows, columns = weight_gate.shape
    step = rows // CHUNKS
    half = CHUNKS // 2
    me = lax.axis_index("zero")
    core = lax.rem(me, 2)
    x = lax.rem(lax.div(me, 2), 2)
    y = lax.div(me, 4)

    def at(yy, xx, cc):
        return (yy * 2 + xx) * 2 + cc

    partner = at(y, x, 1 - core)
    across_x = at(y, 1 - x, core)
    across_y = at(1 - y, x, core)
    across = at(1 - y, 1 - x, core)

    mine = lax.axis_index("tp")
    peers, width = [], 1
    while width < tp:
        bit = lax.rem(lax.div(mine, width), 2)
        peers.append({"tp": mine + width - 2 * width * bit})
        width *= 2
    peers += [{"zero": partner}, {"zero": across_x}, {"zero": across_y}]

    barrier = pltpu.get_barrier_semaphore()
    for peer in peers:
        pl.semaphore_signal(barrier, inc=1, device_id=peer, device_id_type=MESH)
    place = me * tp + mine
    size = norm_train.shape[1]
    gains[place, :, 0:size] = norm_train[...] + norm_step[...]
    pl.semaphore_wait(barrier, len(peers))

    sources = (
        (weight_down, factor_down, other_down),
        (weight_gate, factor_gate, other_gate),
        (weight_up, factor_up, other_up),
    )

    def part(i, owner, c, count=1):
        first = pl.multiple_of(owner * rows + c * step, 16)
        return stack.at[i, pl.ds(first, step * count), :]

    def copy(i, owner, c, peer, send, recv, count=1):
        ref = part(i, owner, c, count)
        return pltpu.make_async_remote_copy(
            src_ref=ref, dst_ref=ref, send_sem=send, recv_sem=recv,
            device_id={"zero": peer}, device_id_type=MESH,
        )

    def on_x(i, owner, c):
        return copy(i, owner, c, across_x, x_send.at[i, c], x_recv.at[i, c])

    def on_y(i, owner, c):
        return copy(i, owner, c, across_y, y_send.at[i, c], y_recv.at[i, c])

    def forward_x(i, owner, c):
        return copy(i, owner, c, across_x, fx_send.at[i, c - half], fx_recv.at[i, c - half])

    def forward_y(i, owner, c):
        return copy(i, owner, c, across_y, fy_send.at[i, c], fy_recv.at[i, c])

    def share(i, slot, owner, c):
        return copy(i, owner, c, partner, p_send.at[slot, i, c], p_recv.at[slot, i, c])

    early, late = range(half), range(half, CHUNKS)
    sent = []

    def go(dma):
        dma.start()
        sent.append(dma)

    for i in range(3):
        weight, factor, other = sources[i]
        first = pl.multiple_of(me * rows, 16)

        @pl.loop(0, columns // LANES)
        def _(t):
            cols = pl.ds(pl.multiple_of(t * LANES, LANES), LANES)
            stack[i, pl.ds(first, rows), cols] = merge_rows(
                weight[:, cols], factor[...], other[:, cols]
            )

        for cx, cy in zip((*early, *late), (*late, *early)):
            go(on_x(i, me, cx))
            go(on_y(i, me, cy))
        for c in range(CHUNKS):
            go(share(i, 0, me, c))

    for k, peer in enumerate(peers):
        width = 1 << k
        block = gains.at[pl.ds(lax.div(place, width) * width, width)]
        dma = pltpu.make_async_remote_copy(
            src_ref=block, dst_ref=block, send_sem=n_send.at[k], recv_sem=n_recv.at[k],
            device_id=peer, device_id_type=MESH,
        )
        dma.start()
        dma.wait_recv()
        sent.append(dma)

    outs = []

    def put(i, slot, owner):
        base = pl.multiple_of(lax.div(owner, 2) * (2 * rows), LANES)
        both = pl.ds(base, 2 * rows)
        if i == 0:

            @pl.loop(0, columns // LANES)
            def _(t):
                cols = pl.ds(pl.multiple_of(t * LANES, LANES), LANES)
                turned[cols, both] = stack[0, both, cols].T

            src, dst = turned.at[:, both], down.at[:, both]
        else:
            src, dst = stack.at[i, both, :], (gate, up)[i - 1].at[both, :]
        dma = pltpu.make_async_copy(src, dst, out_sems.at[i, slot])
        dma.start()
        outs.append(dma)

    def shared(i, slot, owner):
        other_core = owner + partner - me
        for c in range(CHUNKS):
            share(i, slot, other_core, c).wait_recv()
        put(i, slot, owner)

    for i in range(3):
        for c, d in zip(early, late):
            on_x(i, across_x, c).wait_recv()
            go(forward_y(i, across_x, c))
            go(share(i, 1, across_x, c))
            on_y(i, across_y, d).wait_recv()
            go(forward_x(i, across_y, d))
            go(share(i, 2, across_y, d))
        for c, d in zip(early, late):
            on_x(i, across_x, d).wait_recv()
            go(share(i, 1, across_x, d))
            on_y(i, across_y, c).wait_recv()
            go(share(i, 2, across_y, c))
        for slot, owner in ((0, me), (1, across_x), (2, across_y)):
            shared(i, slot, owner)
    for i in range(3):
        for c, d in zip(early, late):
            forward_y(i, across, c).wait_recv()
            go(share(i, 3, across, c))
            forward_x(i, across, d).wait_recv()
            go(share(i, 3, across, d))
        shared(i, 3, across)
    for dma in sent:
        dma.wait_send()
    for dma in outs:
        dma.wait()


def gather(sources, norms, tp):
    rows, columns = sources[0].shape
    stack = (rows * GROUP, columns)
    turned = (columns, rows * GROUP)
    dma = pltpu.SemaphoreType.DMA
    half = CHUNKS // 2
    stages = (GROUP * tp).bit_length() - 1
    return pl.pallas_call(
        functools.partial(gather_kernel, tp),
        out_shape=(
            jax.ShapeDtypeStruct(stack, jnp.bfloat16),
            jax.ShapeDtypeStruct(stack, jnp.bfloat16),
            jax.ShapeDtypeStruct(turned, jnp.bfloat16),
            jax.ShapeDtypeStruct((GROUP * tp, 1, LANES), jnp.float32),
        ),
        in_specs=[pl.BlockSpec(memory_space=pltpu.VMEM)] * 11,
        out_specs=[pl.BlockSpec(memory_space=pl.ANY)] * 3
        + [pl.BlockSpec(memory_space=pltpu.VMEM)],
        scratch_shapes=[
            pltpu.VMEM((3, *stack), jnp.bfloat16),
            pltpu.VMEM(turned, jnp.bfloat16),
            dma((3, 4)),
            dma((stages,)), dma((stages,)),
            dma((3, CHUNKS)), dma((3, CHUNKS)), dma((3, CHUNKS)), dma((3, CHUNKS)),
            dma((3, half)), dma((3, half)), dma((3, half)), dma((3, half)),
            dma((4, 3, CHUNKS)), dma((4, 3, CHUNKS)),
        ],
        compiler_params=pltpu.CompilerParams(
            collective_id=0, has_side_effects=True, vmem_limit_bytes=58 * 2**20
        ),
        name="gather_merged",
    )(*sources, *norms)


def local(
    weight_gate, low_gate, high_gate,
    weight_up, low_up, high_up,
    weight_down, low_down, high_down,
    norm_train, norm_step,
    *, fast, tp,
):
    sources = (
        (weight_down.T, high_down, low_down.T),
        (weight_gate, low_gate.T, high_gate),
        (weight_up, low_up.T, high_up),
    )
    if fast:
        norms = (norm_train[None], norm_step[None])
        ready_gate, ready_up, ready_down, gains = gather(sum(sources, ()), norms, tp)
        serve_norm = gains[:, 0, : norm_train.shape[0]].reshape(-1).astype(jnp.bfloat16)
    else:
        down, gate, up = (merge_rows(*s) for s in sources)
        ready_gate, ready_up, ready_down = (
            lax.all_gather(a, "zero", axis=0, tiled=True) for a in (gate, up, down)
        )
        ready_down = ready_down.T
        serve_norm = lax.all_gather(
            (norm_train + norm_step).astype(jnp.bfloat16), ("zero", "tp"), axis=0, tiled=True
        )
    return (ready_gate, ready_up, ready_down, serve_norm)


def solution(mesh):
    def step(*args):
        zero, tp = mesh.shape["zero"], mesh.shape["tp"]
        rows, columns = args[0].shape[0] // zero, args[0].shape[1] // tp
        fast = (
            zero == GROUP
            and tp & (tp - 1) == 0
            and args[9].shape[0] <= zero * tp * LANES
            and rows % (16 * CHUNKS) == 0
            and columns % LANES == 0
            and 2 * rows % LANES == 0
            and args[6].shape == args[0].shape[::-1]
        )
        return jax.shard_map(
            functools.partial(local, fast=fast, tp=tp),
            mesh=mesh,
            in_specs=(
                P("zero", "tp"), P("zero", None), P(None, "tp"),
                P("zero", "tp"), P("zero", None), P(None, "tp"),
                P("tp", "zero"), P("tp", None), P(None, "zero"),
                P(("zero", "tp")), P(("zero", "tp")),
            ),
            out_specs=(P(None, "tp"), P(None, "tp"), P("tp", None), P()),
            check_vma=False,
        )(*args)

    return step
```

```python
import functools

import jax
import jax.numpy as jnp
from jax import lax
from jax.experimental import pallas as pl
from jax.experimental.pallas import tpu as pltpu
from jax.sharding import PartitionSpec as P

mix_rate = 0.5
MESH = pl.DeviceIdType.MESH
LANES = 128
CHUNKS = 4
GROUP = 8
GRANT = 20 * 2**20


def merge_rows(weight, factor, other):
    product = lax.dot_general(
        factor, other, (((0,), (0,)), ((), ())), preferred_element_type=jnp.float32
    )
    return (weight.astype(jnp.float32) + mix_rate * product).astype(jnp.bfloat16)


def gather_kernel(
    tp,
    weight_down, factor_down, other_down,
    weight_gate, factor_gate, other_gate,
    weight_up, factor_up, other_up,
    norm_train, norm_step,
    gate, up, down, gains, held, weights, w_sems,
    n_send, n_recv,
    x_send, x_recv, y_send, y_recv, fx_send, fx_recv, fy_send, fy_recv, p_send, p_recv,
):
    rows, columns = weight_gate.shape
    step = rows // CHUNKS
    half = CHUNKS // 2
    me = lax.axis_index("zero")
    core = lax.rem(me, 2)
    x = lax.rem(lax.div(me, 2), 2)
    y = lax.div(me, 4)

    def at(yy, xx, cc):
        return (yy * 2 + xx) * 2 + cc

    partner = at(y, x, 1 - core)
    across_x = at(y, 1 - x, core)
    across_y = at(1 - y, x, core)
    across = at(1 - y, 1 - x, core)

    loads = [
        pltpu.make_async_copy(weight, weights.at[i], w_sems.at[i])
        for i, weight in enumerate((weight_down, weight_gate, weight_up))
    ]
    for load in loads:
        load.start()

    mine = lax.axis_index("tp")
    group = [
        at(
            y + dy - 2 * y * dy,
            x + dx - 2 * x * dx,
            core + dc - 2 * core * dc,
        )
        for dy in (0, 1) for dx in (0, 1) for dc in (0, 1) if dy + dx + dc
    ]
    peers, width = [{"zero": peer} for peer in group], 1
    while width < tp:
        bit = lax.rem(lax.div(mine, width), 2)
        peers.append({"tp": mine + width - 2 * width * bit})
        width *= 2

    barrier = pltpu.get_barrier_semaphore()
    for peer in peers:
        pl.semaphore_signal(barrier, inc=1, device_id=peer, device_id_type=MESH)
    place = mine * GROUP + me
    size = norm_train.shape[1]
    gains[place, :, 0:size] = norm_train[...] + norm_step[...]
    pl.semaphore_wait(barrier, len(peers))

    def pass_gains(k, first, count):
        block = gains.at[pl.ds(first, count)]
        dma = pltpu.make_async_remote_copy(
            src_ref=block, dst_ref=block, send_sem=n_send.at[k], recv_sem=n_recv.at[k],
            device_id=peers[k], device_id_type=MESH,
        )
        dma.start()
        return dma

    passed = [pass_gains(k, place, 1) for k in range(len(group))]

    stacks = (held, gate, up)
    factors = (
        (factor_down, other_down), (factor_gate, other_gate), (factor_up, other_up)
    )

    def part(i, owner, c, count=1):
        first = pl.multiple_of(owner * rows + c * step, 16)
        return stacks[i].at[pl.ds(first, step * count), :]

    def copy(i, owner, c, peer, send, recv, count=1):
        ref = part(i, owner, c, count)
        return pltpu.make_async_remote_copy(
            src_ref=ref, dst_ref=ref, send_sem=send, recv_sem=recv,
            device_id={"zero": peer}, device_id_type=MESH,
        )

    def on_x(i, owner, c):
        return copy(i, owner, c, across_x, x_send.at[i, c], x_recv.at[i, c])

    def on_y(i, owner, c):
        return copy(i, owner, c, across_y, y_send.at[i, c], y_recv.at[i, c])

    def forward_x(i, owner, c):
        return copy(i, owner, c, across_x, fx_send.at[i, c - half], fx_recv.at[i, c - half])

    def forward_y(i, owner, c):
        return copy(i, owner, c, across_y, fy_send.at[i, c], fy_recv.at[i, c])

    def share(i, slot, owner, c):
        return copy(i, owner, c, partner, p_send.at[slot, i, c], p_recv.at[slot, i, c])

    early, late = range(half), range(half, CHUNKS)
    sent = []

    def go(dma):
        dma.start()
        sent.append(dma)

    for i in range(3):
        factor, other = factors[i]
        loads[i].wait()
        first = pl.multiple_of(me * rows, 16)

        @pl.loop(0, columns // LANES)
        def _(t):
            cols = pl.ds(pl.multiple_of(t * LANES, LANES), LANES)
            stacks[i][pl.ds(first, rows), cols] = merge_rows(
                weights[i, :, cols], factor[...], other[:, cols]
            )

        for cx, cy in zip((*early, *late), (*late, *early)):
            go(on_x(i, me, cx))
            go(on_y(i, me, cy))
        for c in range(CHUNKS):
            go(share(i, 0, me, c))

    for dma in passed:
        dma.wait_recv()
    for k in range(len(group), len(peers)):
        width = 1 << (k - len(group))
        passed.append(pass_gains(k, lax.div(mine, width) * (width * GROUP), width * GROUP))
        passed[-1].wait_recv()
    sent += passed

    def turn(owner):
        base = pl.multiple_of(lax.div(owner, 2) * (2 * rows), LANES)

        @pl.loop(0, columns // LANES)
        def _(t):
            cols = pl.ds(pl.multiple_of(t * LANES, LANES), LANES)
            down[cols, pl.ds(base, 2 * rows)] = held[pl.ds(base, 2 * rows), cols].T

    def shared(i, slot, owner):
        other_core = owner + partner - me
        for c in range(CHUNKS):
            share(i, slot, other_core, c).wait_recv()

    for i in range(3):
        for c, d in zip(early, late):
            on_x(i, across_x, c).wait_recv()
            go(forward_y(i, across_x, c))
            go(share(i, 1, across_x, c))
            on_y(i, across_y, d).wait_recv()
            go(forward_x(i, across_y, d))
            go(share(i, 2, across_y, d))
        for c, d in zip(early, late):
            on_x(i, across_x, d).wait_recv()
            go(share(i, 1, across_x, d))
            on_y(i, across_y, c).wait_recv()
            go(share(i, 2, across_y, c))
        for slot, owner in ((0, me), (1, across_x), (2, across_y)):
            shared(i, slot, owner)
            if i == 0:
                turn(owner)
    for i in range(3):
        for c, d in zip(early, late):
            forward_y(i, across, c).wait_recv()
            go(share(i, 3, across, c))
            forward_x(i, across, d).wait_recv()
            go(share(i, 3, across, d))
        if i == 0:
            shared(i, 3, across)
            turn(across)
    for i in (1, 2):
        shared(i, 3, across)
    for dma in sent:
        dma.wait_send()


def gather(sources, norms, tp):
    rows, columns = sources[0].shape
    stack = (rows * GROUP, columns)
    turned = (columns, rows * GROUP)
    dma = pltpu.SemaphoreType.DMA
    half = CHUNKS // 2
    stages = GROUP - 1 + tp.bit_length() - 1
    anywhere = pl.BlockSpec(memory_space=pl.ANY)
    held = pl.BlockSpec(memory_space=pltpu.VMEM)
    return pl.pallas_call(
        functools.partial(gather_kernel, tp),
        out_shape=(
            pltpu.VMEM(stack, jnp.bfloat16),
            pltpu.VMEM(stack, jnp.bfloat16),
            pltpu.VMEM(turned, jnp.bfloat16),
            pltpu.VMEM((GROUP * tp, 1, LANES), jnp.float32),
        ),
        in_specs=[anywhere, held, held] * 3 + [held, held],
        out_specs=[pl.BlockSpec(memory_space=pltpu.VMEM)] * 4,
        scratch_shapes=[
            pltpu.VMEM(stack, jnp.bfloat16),
            pltpu.VMEM((3, rows, columns), jnp.bfloat16),
            dma((3,)),
            dma((stages,)), dma((stages,)),
            dma((3, CHUNKS)), dma((3, CHUNKS)), dma((3, CHUNKS)), dma((3, CHUNKS)),
            dma((3, half)), dma((3, half)), dma((3, half)), dma((3, half)),
            dma((4, 3, CHUNKS)), dma((4, 3, CHUNKS)),
        ],
        compiler_params=pltpu.CompilerParams(
            collective_id=0, has_side_effects=True, vmem_limit_bytes=GRANT
        ),
        name="gather_merged",
    )(*sources, *norms)


def store_kernel(gate, up, down, gains, gate_out, up_out, down_out, gains_out, sems):
    pieces = 4
    copies = [pltpu.make_async_copy(gains, gains_out, sems.at[3, 0])]
    copies[0].start()
    for i, (src, dst) in enumerate(((gate, gate_out), (up, up_out), (down, down_out))):
        size = src.shape[0] // pieces
        for k in range(pieces):
            at = pl.ds(k * size, size)
            copies.append(pltpu.make_async_copy(src.at[at, :], dst.at[at, :], sems.at[i, k]))
            copies[-1].start()
    for copy in copies:
        copy.wait()


def store(*held):
    held = [pltpu.with_memory_space_constraint(a, pltpu.VMEM) for a in held]
    return pl.pallas_call(
        store_kernel,
        out_shape=tuple(jax.ShapeDtypeStruct(a.shape, a.dtype) for a in held),
        in_specs=[pl.BlockSpec(memory_space=pltpu.VMEM)] * 4,
        out_specs=[pl.BlockSpec(memory_space=pl.ANY)] * 4,
        scratch_shapes=[pltpu.SemaphoreType.DMA((4, 4))],
        compiler_params=pltpu.CompilerParams(vmem_limit_bytes=GRANT),
        name="store_merged",
    )(*held)


def local(
    weight_gate, low_gate, high_gate,
    weight_up, low_up, high_up,
    weight_down, low_down, high_down,
    norm_train, norm_step,
    *, fast, tp,
):
    sources = (
        (weight_down.T, high_down, low_down.T),
        (weight_gate, low_gate.T, high_gate),
        (weight_up, low_up.T, high_up),
    )
    if fast:
        norms = (norm_train[None], norm_step[None])
        ready_gate, ready_up, ready_down, gains = store(*gather(sum(sources, ()), norms, tp))
        gains = gains[:, 0, : norm_train.shape[0]].reshape(tp, GROUP, -1)
        serve_norm = gains.transpose(1, 0, 2).reshape(-1).astype(jnp.bfloat16)
    else:
        down, gate, up = (merge_rows(*s) for s in sources)
        ready_gate, ready_up, ready_down = (
            lax.all_gather(a, "zero", axis=0, tiled=True) for a in (gate, up, down)
        )
        ready_down = ready_down.T
        serve_norm = lax.all_gather(
            (norm_train + norm_step).astype(jnp.bfloat16), ("zero", "tp"), axis=0, tiled=True
        )
    return (ready_gate, ready_up, ready_down, serve_norm)


def solution(mesh):
    def step(*args):
        zero, tp = mesh.shape["zero"], mesh.shape["tp"]
        rows, columns = args[0].shape[0] // zero, args[0].shape[1] // tp
        fast = (
            zero == GROUP
            and tp & (tp - 1) == 0
            and args[9].shape[0] <= zero * tp * LANES
            and rows % (16 * CHUNKS) == 0
            and columns % LANES == 0
            and 2 * rows % LANES == 0
            and args[6].shape == args[0].shape[::-1]
        )
        return jax.shard_map(
            functools.partial(local, fast=fast, tp=tp),
            mesh=mesh,
            in_specs=(
                P("zero", "tp"), P("zero", None), P(None, "tp"),
                P("zero", "tp"), P("zero", None), P(None, "tp"),
                P("tp", "zero"), P("tp", None), P(None, "zero"),
                P(("zero", "tp")), P(("zero", "tp")),
            ),
            out_specs=(P(None, "tp"), P(None, "tp"), P("tp", None), P()),
            check_vma=False,
        )(*args)

    return step
```
